32 devices in a mesh: img: 4 (over x, core), head: 2 (over y), txt: 4 (over z).
Axes of the slice: x: 2, y: 2, z: 4, core: 2. Of those that a mesh axis runs over, the one named last changes fastest.
Arguments:
- image_feats: bfloat16 [4096, 7680], P(('img', 'txt'), 'head'), may hold values from -6 to 6
- key_weight: bfloat16 [7680, 512], P('head'), may hold values from -0.0625 to 0.0625
- value_weight: bfloat16 [7680, 512], P('head'), may hold values from -0.0625 to 0.0625
- queries: bfloat16 [1024, 4096], P('txt', 'head'), may hold values from -21 to 21
- grad_out: bfloat16 [1024, 4096], P('txt', 'head'), may hold values from -768 to 768
- tile_image: int32 [32], P('img'), may hold values from 0 to 7, never falling along the last dimension, each value on 1 to 8 neighbouring positions
- text_sees: int32 [8, 8], replicated, may hold values from 0 to 1, as said below
Outputs:
- attn_out: bfloat16 [1024, 4096], P('txt', 'head')
- grad_feats: bfloat16 [4096, 7680], P(('img', 'txt'), 'head')
The draws below stay inside these ranges and needn't reach their ends.
Inputs may be any that keep to these rules, and one draw needn't show every extreme that they name: `text_sees`: every row holds at least one 1.
All inputs are finite; a program needn't handle non-finite values.
Results may differ from the reference program's by a relative error of at most 0.012.
The reference program's roundings to bfloat16 on the way (of `weights`) count: a program that leaves them out, or rounds other values in their place, can miss the bound.
Values may be sent and summed in bfloat16 or wider, within the bound.
A program may use at most 128 MiB of HBM per device.

```python
import math
import jax
import jax.numpy as jnp
import numpy as np
from jax import lax

DV = 7680
HD = 128
KVH = 4
QH = 32
TILE = 128
TBLK = 128
IMAGES = 8
IMG = 4096
TXT = 1024
TILES = 32
TBLKS = 8
MOST = 8


def draw_queries(key, part):
    key_base, key_scale = jax.random.split(key, 2)
    shape = (TXT, QH * HD)
    row_scale = jnp.exp(jax.random.uniform(key_scale, (TXT, 1), jnp.float32, math.log(0.5), math.log(4.0)))
    base_values = jnp.clip(jax.random.normal(key_base, shape, jnp.float32), -4.0, 4.0)
    return (base_values * row_scale).astype(jnp.bfloat16)


def draw_text_sees(key, part):
    random_bits = jax.random.randint(key, (TBLKS, IMAGES), 0, 2)
    forced = jax.random.randint(jax.random.fold_in(key, 1), (TBLKS, 1), 0, IMAGES)
    forced_hit = (jnp.arange(IMAGES)[None, :] == forced).astype(jnp.int32)
    return jnp.maximum(random_bits, forced_hit).astype(jnp.int32)


def block_scale(own_key, dims, pieces, low, high):
    def one(axis_at, parts):
        steps = jax.random.uniform(jax.random.fold_in(jax.random.fold_in(own_key, 6), axis_at), (parts,), jnp.float32, low / len(pieces), high / len(pieces))
        return jnp.repeat(jnp.exp(steps), dims[axis_at] // parts).reshape((-1,) + (1,) * (len(dims) - axis_at - 1))

    loudness = one(*pieces[0])
    for cut in pieces[1:]:
        loudness = loudness * one(*cut)
    return loudness


def profile(count, total, limit, lean):
    weights = [(1 << 20) // math.isqrt(rank ** lean) + 1 for rank in range(2, count + 1)]
    surplus, counts = total - limit - (count - 1), [1] * (count - 1)
    while surplus > 0:
        movable = [i for i in range(count - 1) if counts[i] < limit]
        pool, remaining = sum([weights[i] for i in movable]), surplus
        for i in movable:
            more = min(limit - counts[i], max(1, remaining * weights[i] // pool), surplus)
            counts[i] = counts[i] + more
            surplus = surplus - more
    return np.array([limit] + counts)


def ragged_sizes(key, number_of, total, most, slope):
    if number_of == 2:
        one = jax.random.randint(key, (), max(1, total - most), min(most, total - 1) + 1)
        return jnp.stack([one, total - one])
    lengths = jnp.asarray(profile(number_of, total, most, slope), jnp.int32)
    pairs = (number_of - 1) // 2
    giver, sink = lengths[1:1 + 2 * pairs:2], lengths[2:2 + 2 * pairs:2]
    slack = jnp.minimum(giver - 1, most - sink)
    moved = jax.random.randint(jax.random.fold_in(key, 1), (pairs,), 0, 1 << 20) % (slack + 1)
    lengths = lengths.at[1:1 + 2 * pairs:2].set(giver - moved).at[2:2 + 2 * pairs:2].set(sink + moved)
    return lengths[jax.random.permutation(jax.random.fold_in(key, 2), number_of)]


def scatter_about(key, dims, deviation, limit, shards=(), kind=jnp.bfloat16):
    loudness = block_scale(key, dims, shards, -0.22, 0.18) if shards else 1.0
    values = jax.random.normal(key, dims, jnp.float32) * deviation * loudness
    return jnp.minimum(jnp.maximum(values, -limit), limit).astype(kind)


def setup_inputs(seed: int = 0) -> dict:
    splits = jax.random.split(jax.random.key(seed), 8)
    image_feats = scatter_about(splits[0], (IMG, DV), 1.0, 6.0, ((0, 16), (1, 2)))
    key_weight = scatter_about(splits[1], (DV, KVH * HD), DV ** -0.5, 0.0625, ((0, 2),))
    value_weight = scatter_about(splits[2], (DV, KVH * HD), DV ** -0.5, 0.0625, ((0, 2),))
    queries = draw_queries(jax.random.fold_in(splits[7], 71), 0)
    grad_out = scatter_about(splits[4], (TXT, QH * HD), 128.0, 768.0, ((0, 4), (1, 2)))
    tile_image = jnp.searchsorted(jnp.cumsum(ragged_sizes(splits[5], IMAGES, TILES, MOST, 2)), jnp.arange(TILES), side="right").astype(jnp.int32)
    text_sees = draw_text_sees(jax.random.fold_in(splits[7], 71), 0)
    return dict(image_feats=image_feats, key_weight=key_weight, value_weight=value_weight, queries=queries, grad_out=grad_out, tile_image=tile_image, text_sees=text_sees)


def attend_one(query, grad_head, key_head, value_head, allowed, scale_factor):
    scores = jnp.dot(query, key_head.T, preferred_element_type=jnp.float32) * scale_factor
    masked = jnp.where(allowed, scores, -1e+30)
    row_max = lax.optimization_barrier(jnp.max(masked, axis=1))
    weights = jnp.exp(masked - row_max[:, None]).astype(jnp.bfloat16)
    totals = lax.optimization_barrier(jnp.sum(weights, axis=1, dtype=jnp.float32))
    numerator = jnp.dot(weights, value_head, preferred_element_type=jnp.float32)
    output = (numerator / totals[:, None]).astype(jnp.bfloat16)
    log_total = row_max + jnp.log(totals)
    row_delta = lax.optimization_barrier(jnp.sum(grad_head.astype(jnp.float32) * output.astype(jnp.float32), axis=1))
    probabilities = jnp.exp(masked - log_total[:, None])
    grad_probs = jnp.dot(grad_head, value_head.T, preferred_element_type=jnp.float32)
    grad_scores = (probabilities * (grad_probs - row_delta[:, None]) * scale_factor).astype(jnp.bfloat16)
    value_grad = jnp.dot(probabilities.astype(jnp.bfloat16).T, grad_head, preferred_element_type=jnp.float32)
    key_grad = jnp.dot(grad_scores.T, query, preferred_element_type=jnp.float32)
    return (output, key_grad, value_grad)

def reference(image_feats, key_weight, value_weight, queries, grad_out, tile_image, text_sees):
    scale_factor = 1.0 / math.sqrt(HD)
    keys = jnp.dot(image_feats, key_weight, preferred_element_type=jnp.float32).astype(jnp.bfloat16)
    values = jnp.dot(image_feats, value_weight, preferred_element_type=jnp.float32).astype(jnp.bfloat16)
    block_allowed = text_sees[:, tile_image]
    allowed = jnp.repeat(jnp.repeat(block_allowed, TBLK, axis=0), TILE, axis=1) > 0
    repeats = QH // KVH
    query_heads = queries.reshape(TXT, KVH, repeats, HD).transpose(1, 2, 0, 3)
    grad_heads = grad_out.reshape(TXT, KVH, repeats, HD).transpose(1, 2, 0, 3)
    key_heads = keys.reshape(IMG, KVH, HD).transpose(1, 0, 2)
    value_heads = values.reshape(IMG, KVH, HD).transpose(1, 0, 2)

    def per_group(operands):
        group_queries, group_grads, key_head, value_head = operands

        def per_query(carry, pair):
            output, key_grad, value_grad = attend_one(pair[0], pair[1], key_head, value_head, allowed, scale_factor)
            return ((carry[0] + key_grad, carry[1] + value_grad), output)
        start = (jnp.zeros((IMG, HD), jnp.float32), jnp.zeros((IMG, HD), jnp.float32))
        summed, outputs = lax.scan(per_query, start, (group_queries, group_grads))
        return (outputs, summed[0], summed[1])
    outputs, key_grad, value_grad = lax.map(per_group, (query_heads, grad_heads, key_heads, value_heads))
    attn_out = outputs.transpose(2, 0, 1, 3).reshape(TXT, QH * HD)
    key_grad = key_grad.transpose(1, 0, 2).reshape(IMG, KVH * HD).astype(jnp.bfloat16)
    value_grad = value_grad.transpose(1, 0, 2).reshape(IMG, KVH * HD).astype(jnp.bfloat16)
    grad_feats = jnp.dot(key_grad, key_weight.T, preferred_element_type=jnp.float32)
    grad_feats = grad_feats + jnp.dot(value_grad, value_weight.T, preferred_element_type=jnp.float32)
    return (attn_out, grad_feats.astype(jnp.bfloat16))
```

```python
import functools
import math

import jax
import jax.numpy as jnp
from jax import lax
from jax.experimental import pallas as pl
from jax.experimental.pallas import tpu as pltpu
from jax.sharding import PartitionSpec as P

HD = 128
TILE = 128
TBLK = 128
MESH = pl.DeviceIdType.MESH
UNROLL = 4
LOG2E = 1.4426950408889634
NT = (((1,), (1,)), ((), ()))
F32 = jnp.float32
BF16 = jnp.bfloat16


def build_mask(text_sees, tile_image, text_count):
    blocks_total, images_total = text_sees.shape
    text_rows = lax.axis_index("txt") * text_count + jnp.arange(text_count, dtype=jnp.int32)
    block_onehot = (
        (text_rows // TBLK)[:, None] == jnp.arange(blocks_total, dtype=jnp.int32)[None, :]
    ).astype(F32)
    tile_onehot = (
        tile_image[:, None] == jnp.arange(images_total, dtype=jnp.int32)[None, :]
    ).astype(F32)
    tile_sees = jnp.dot(tile_onehot, text_sees.astype(F32).T)
    return jnp.dot(tile_sees, block_onehot.T)


def partner(me, step, count):
    if count & (count - 1):
        return lax.rem(me + step, count)
    other, bit = me, 1
    while bit < count:
        if step & bit:
            other = other + bit - 2 * bit * (lax.rem(other // bit, 2))
        bit *= 2
    return other


def receive_from(me, step, count):
    if count & (count - 1):
        return lax.rem(me - step + count, count)
    return partner(me, step, count)


def kernel(
    sizes,
    feats, kw, vw, q, g, mask,
    attn, dfeats,
    psend, precv, pacc, kvbuf, vtb, sbuf, numt, mst, tst, stbuf, lse, dlt, cown,
    osend, orecv, aout, gsend, grecv, gown, gacc, hall, grelay, facc,
    p_ss, p_rs, kv_ss, kv_rs, st_ss, st_rs, o_ss, o_rs, a_ss, a_rs, g_ss, g_rs, h_ss, h_rs,
    r_ss, gr_ss, gr_rs,
):
    ni, nh, nt = sizes
    img, hd, txt = lax.axis_index("img"), lax.axis_index("head"), lax.axis_index("txt")
    rows = feats.shape[0]
    groups = kvbuf.shape[1] // 2
    own_cols = groups * HD
    heads = q.shape[1] // HD
    reps = heads // groups
    block_tiles = rows // TILE
    share = osend.shape[1]
    relay = nt == 4
    inner = jnp.logical_or(txt == 1, txt == 2)
    outer = jnp.logical_not(inner)
    scale = 1.0 / math.sqrt(HD)
    unroll = math.gcd(UNROLL, reps)

    barrier = pltpu.get_barrier_semaphore()
    for step in range(1, nh):
        pl.semaphore_signal(barrier, inc=1, device_id={"head": lax.rem(hd + step, nh)}, device_id_type=MESH)
    for step in range(1, nt):
        pl.semaphore_signal(barrier, inc=1, device_id={"txt": lax.rem(txt + step, nt)}, device_id_type=MESH)
    for step in range(1, ni):
        pl.semaphore_signal(barrier, inc=1, device_id={"img": lax.rem(img + step, ni)}, device_id_type=MESH)
    pl.semaphore_wait(barrier, nh - 1 + nt - 1 + ni - 1)

    def remote(src, dst, ss, rs, axis, index):
        return pltpu.make_async_remote_copy(
            src_ref=src, dst_ref=dst, send_sem=ss, recv_sem=rs,
            device_id={axis: index}, device_id_type=MESH,
        )

    p_copies = []
    for step in range(1, nh):
        dest = lax.rem(hd + step, nh)
        cols = pl.ds(pl.multiple_of(dest * own_cols, own_cols), own_cols)
        for part, weight in enumerate((kw, vw)):
            psend[step - 1, part] = jnp.dot(
                feats[...], weight[:, cols], preferred_element_type=F32
            ).astype(BF16)
            copy = remote(
                psend.at[step - 1, part], precv.at[step - 1, part],
                p_ss.at[step - 1, part], p_rs.at[step - 1, part], "head", dest,
            )
            copy.start()
            p_copies.append(copy)
    cols = pl.ds(pl.multiple_of(hd * own_cols, own_cols), own_cols)
    for part, weight in enumerate((kw, vw)):
        pacc[part] = jnp.dot(feats[...], weight[:, cols], preferred_element_type=F32)
    kv_copies, relayed = [], []
    for part in range(2):
        total = pacc[part]
        for step in range(1, nh):
            p_copies[(step - 1) * 2 + part].wait_recv()
            total = total + precv[step - 1, part].astype(F32)
        total = total.astype(BF16)
        for group in range(groups):
            kvbuf[txt, part * groups + group] = total[:, group * HD : (group + 1) * HD]
        mine = kvbuf.at[txt, pl.ds(part * groups, groups)]
        for step in range(1, nt):
            copy = remote(
                mine, mine, kv_ss.at[step - 1, part], kv_rs.at[step - 1, part],
                "txt", partner(txt, step, nt),
            )
            if relay and step == 3:
                pl.when(inner)(copy.start)
            else:
                copy.start()
            kv_copies.append(copy)

    for step in range(nt):
        block = receive_from(txt, step, nt)
        if step:
            for part in range(2):
                kv_copies[part * (nt - 1) + step - 1].wait_recv()
                if relay and step == 2:
                    passed = kvbuf.at[block, pl.ds(part * groups, groups)]
                    copy = remote(
                        passed, passed, r_ss.at[part], kv_rs.at[2, part], "txt", partner(txt, 1, nt)
                    )
                    pl.when(inner)(copy.start)
                    relayed.append(copy)
        for group in range(groups):
            vtb[group] = kvbuf[block, groups + group].astype(F32).T.astype(BF16)

        def forward(turn, _, step=step, block=block):
            picked = [turn * unroll + i for i in range(unroll)]
            spans = [pl.ds(pl.multiple_of(head * HD, HD), HD) for head in picked]
            at = [pl.ds(head, 1) for head in picked]
            group = turn * unroll // reps
            keys, values_t = kvbuf[block, group], vtb[group]
            allowed = [
                mask[pl.ds(block * block_tiles + tile, 1), :] > 0.5 for tile in range(block_tiles)
            ]
            if step:
                before = [mst[row, :] for row in at]
                sums = [tst[row, :] for row in at]
                numers = [numt[head] for head in picked]
            kept, tops, totals, outs = [], [], [], []
            for i in range(unroll):
                scores = lax.dot_general(keys, q[:, spans[i]], NT, preferred_element_type=F32)
                scores = scores * (scale * LOG2E)
                masked = jnp.concatenate(
                    [
                        jnp.where(allowed[tile], scores[tile * TILE : (tile + 1) * TILE], -1e30)
                        for tile in range(block_tiles)
                    ],
                    axis=0,
                )
                top = jnp.max(masked, axis=0, keepdims=True)
                if step:
                    top = jnp.maximum(top, before[i])
                kept.append(masked)
                tops.append(top)
            for i in range(unroll):
                weights = jnp.exp2(kept[i] - tops[i]).astype(BF16)
                total = jnp.sum(weights.astype(F32), axis=0, keepdims=True)
                numer = jnp.dot(values_t, weights, preferred_element_type=F32)
                if step:
                    shrink = jnp.exp2(before[i] - tops[i])
                    total = total + sums[i] * shrink
                    numer = numer + numers[i] * shrink
                totals.append(total)
                outs.append(numer)
            for i in range(unroll):
                sbuf[step * heads + picked[i]] = kept[i]
                mst[at[i], :] = tops[i]
                tst[at[i], :] = totals[i]
                numt[picked[i]] = outs[i]
            return 0

        lax.fori_loop(0, heads // unroll, forward, 0)

    def deltas(head, _):
        cols = pl.ds(pl.multiple_of(head * HD, HD), HD)
        grad_t = g[:, cols].astype(F32).T
        row = pl.ds(head, 1)
        stbuf[img, 0, row, :] = mst[row, :]
        stbuf[img, 1, row, :] = tst[row, :]
        stbuf[img, 2, row, :] = jnp.sum(grad_t * numt[head], axis=0, keepdims=True)
        return 0

    lax.fori_loop(0, heads, deltas, 0)
    st_copies = []
    for step in range(1, ni):
        copy = remote(
            stbuf.at[img], stbuf.at[img], st_ss.at[step - 1], st_rs.at[step - 1],
            "img", lax.rem(img + step, ni),
        )
        copy.start()
        st_copies.append(copy)
    for copy in st_copies:
        copy.wait_recv()
    top = stbuf[0, 0]
    for i in range(1, ni):
        top = jnp.maximum(top, stbuf[i, 0])
    total = jnp.zeros_like(top)
    delta = jnp.zeros_like(top)
    for i in range(ni):
        factor = jnp.exp2(stbuf[i, 0] - top)
        total = total + factor * stbuf[i, 1]
        delta = delta + factor * stbuf[i, 2]
    lse[...] = top + jnp.log(total) * LOG2E
    dlt[...] = delta / total
    cown[...] = jnp.exp2(stbuf[img, 0] - top) / total

    def outputs(head, _):
        cols = pl.ds(pl.multiple_of(head * HD, HD), HD)
        piece = (numt[head] * cown[pl.ds(head, 1), :]).T.astype(BF16)
        for i in range(ni):
            osend[i, :, cols] = piece[i * share : (i + 1) * share]
        return 0

    lax.fori_loop(0, heads, outputs, 0)
    o_copies = []
    for step in range(1, ni):
        dest = lax.rem(img + step, ni)
        copy = remote(
            osend.at[dest], orecv.at[step - 1], o_ss.at[step - 1], o_rs.at[step - 1], "img", dest
        )
        copy.start()
        o_copies.append(copy)

    g_copies = []
    for step in range(nt - 1, -1, -1):
        block = receive_from(txt, step, nt)

        for group in range(groups):

            def backward(turn, _, step=step, block=block, group=group):
                picked = [group * reps + turn * unroll + i for i in range(unroll)]
                spans = [pl.ds(pl.multiple_of(head * HD, HD), HD) for head in picked]
                at = [pl.ds(head, 1) for head in picked]
                values = kvbuf[block, groups + group]
                key_grad, value_grad = gacc[0], gacc[1]
                grad_probs = [
                    lax.dot_general(values, g[:, cols], NT, preferred_element_type=F32)
                    for cols in spans
                ]
                for i in range(unroll):
                    probs = jnp.exp2(sbuf[step * heads + picked[i]] - lse[at[i], :])
                    grad_scores = (probs * (grad_probs[i] - dlt[at[i], :])).astype(BF16)
                    key_grad = key_grad + jnp.dot(
                        grad_scores, q[:, spans[i]], preferred_element_type=F32
                    )
                    value_grad = value_grad + jnp.dot(
                        probs.astype(BF16), g[:, spans[i]], preferred_element_type=F32
                    )
                gacc[0] = key_grad
                gacc[1] = value_grad
                return 0

            gacc[...] = jnp.zeros_like(gacc)
            lax.fori_loop(0, reps // unroll, backward, 0)
            if relay and step == 2:
                gown[group] = gacc[0] * scale
                gown[groups + group] = gacc[1]
            elif step:
                gsend[step - 1, group] = (gacc[0] * scale).astype(BF16)
                gsend[step - 1, groups + group] = gacc[1].astype(BF16)
            else:
                gown[group] = gacc[0] * scale
                gown[groups + group] = gacc[1]
        if relay and step == 2:

            def joined():
                relay_up.wait_recv()
                for part in range(2 * groups):
                    gsend[1, part] = (gown[part] + grelay[part].astype(F32)).astype(BF16)

            def alone():
                for part in range(2 * groups):
                    gsend[1, part] = gown[part].astype(BF16)

            pl.when(inner)(joined)
            pl.when(outer)(alone)
        if step:
            copy = remote(
                gsend.at[step - 1], grecv.at[step - 1], g_ss.at[step - 1], g_rs.at[step - 1],
                "txt", block,
            )
            if relay and step == 3:
                relay_up = remote(
                    gsend.at[2], grelay, gr_ss.at[0], gr_rs.at[0], "txt", partner(txt, 1, nt)
                )
                pl.when(inner)(copy.start)
                pl.when(outer)(relay_up.start)
                far = copy
            else:
                copy.start()
                g_copies.append(copy)

    for copy in o_copies:
        copy.wait_recv()
    rows_sum = osend[img].astype(F32)
    for step in range(1, ni):
        rows_sum = rows_sum + orecv[step - 1].astype(F32)
    aout[img] = rows_sum.astype(BF16)
    a_copies = []
    for step in range(1, ni):
        copy = remote(
            aout.at[img], aout.at[img], a_ss.at[step - 1], a_rs.at[step - 1],
            "img", lax.rem(img + step, ni),
        )
        copy.start()
        a_copies.append(copy)

    for copy in g_copies:
        copy.wait_recv()
    for part in range(2 * groups):
        total = gown[part]
        for step in range(1, 3 if relay else nt):
            total = total + grecv[step - 1, part].astype(F32)
        gown[part] = total
    if relay:

        def add_far():
            far.wait_recv()
            for part in range(2 * groups):
                gown[part] = gown[part] + grecv[2, part].astype(F32)

        pl.when(inner)(add_far)
    for part in range(2 * groups):
        hall[hd, part] = gown[part].astype(BF16)
    h_copies = []
    for step in range(1, nh):
        copy = remote(
            hall.at[hd], hall.at[hd], h_ss.at[step - 1], h_rs.at[step - 1],
            "head", lax.rem(hd + step, nh),
        )
        copy.start()
        h_copies.append(copy)
    width = feats.shape[1]
    chunk = math.gcd(width, 768)

    def features(owner):
        cols = pl.ds(pl.multiple_of(owner * own_cols, own_cols), own_cols)
        key_part = jnp.concatenate([hall[owner, i] for i in range(groups)], axis=1)
        value_part = jnp.concatenate([hall[owner, groups + i] for i in range(groups)], axis=1)

        def part(at):
            span = pl.ds(pl.multiple_of(at * chunk, chunk), chunk)
            return span, lax.dot_general(
                key_part, kw[span, cols], NT, preferred_element_type=F32
            ) + lax.dot_general(value_part, vw[span, cols], NT, preferred_element_type=F32)

        return part

    own_part = features(hd)

    def own_features(at, _):
        span, value = own_part(at)
        facc[:, span] = value
        return 0

    lax.fori_loop(0, width // chunk, own_features, 0)
    for step in range(1, nh):
        h_copies[step - 1].wait_recv()
        other_part = features(lax.rem(hd - step + nh, nh))

        def other_features(at, _, step=step, other_part=other_part):
            span, value = other_part(at)
            value = facc[:, span] + value
            if step == nh - 1:
                dfeats[:, span] = value.astype(BF16)
            else:
                facc[:, span] = value
            return 0

        lax.fori_loop(0, width // chunk, other_features, 0)

    for copy in a_copies:
        copy.wait_recv()
    for i in range(ni):
        attn[i] = aout[i]
    near = [copy for at, copy in enumerate(kv_copies) if not (relay and at % (nt - 1) == 2)]
    for copy in p_copies + near + st_copies + o_copies + g_copies + a_copies + h_copies:
        copy.wait_send()
    if relay:

        def inner_sends():
            for copy in [kv_copies[2], kv_copies[5], far] + relayed:
                copy.wait_send()

        pl.when(inner)(inner_sends)
        pl.when(outer)(relay_up.wait_send)


def shards(sizes, image_feats, key_weight, value_weight, queries, grad_out, tile_image, text_sees):
    ni, nh, nt = sizes
    rows = image_feats.shape[0]
    text, width = queries.shape
    heads = width // HD
    own_cols = key_weight.shape[1] // nh
    groups = own_cols // HD
    share = text // ni
    mask = build_mask(text_sees, tile_image, text)
    dma = pltpu.SemaphoreType.DMA
    vmem = pl.BlockSpec(memory_space=pltpu.VMEM)
    attn, grad_feats = pl.pallas_call(
        functools.partial(kernel, sizes),
        out_shape=(
            jax.ShapeDtypeStruct((ni, share, width), BF16),
            jax.ShapeDtypeStruct(image_feats.shape, BF16),
        ),
        in_specs=[vmem] * 6,
        out_specs=(vmem, vmem),
        scratch_shapes=[
            pltpu.VMEM((nh - 1, 2, rows, own_cols), BF16),
            pltpu.VMEM((nh - 1, 2, rows, own_cols), BF16),
            pltpu.VMEM((2, rows, own_cols), F32),
            pltpu.VMEM((nt, 2 * groups, rows, HD), BF16),
            pltpu.VMEM((groups, HD, rows), BF16),
            pltpu.VMEM((nt * heads, rows, text), F32),
            pltpu.VMEM((heads, HD, text), F32),
            pltpu.VMEM((heads, text), F32),
            pltpu.VMEM((heads, text), F32),
            pltpu.VMEM((ni, 3, heads, text), F32),
            pltpu.VMEM((heads, text), F32),
            pltpu.VMEM((heads, text), F32),
            pltpu.VMEM((heads, text), F32),
            pltpu.VMEM((ni, share, width), BF16),
            pltpu.VMEM((ni - 1, share, width), BF16),
            pltpu.VMEM((ni, share, width), BF16),
            pltpu.VMEM((nt - 1, 2 * groups, rows, HD), BF16),
            pltpu.VMEM((nt - 1, 2 * groups, rows, HD), BF16),
            pltpu.VMEM((2 * groups, rows, HD), F32),
            pltpu.VMEM((2, rows, HD), F32),
            pltpu.VMEM((nh, 2 * groups, rows, HD), BF16),
            pltpu.VMEM((2 * groups, rows, HD), BF16),
            pltpu.VMEM((rows, image_feats.shape[1]), F32),
            dma((nh - 1, 2)), dma((nh - 1, 2)),
            dma((nt - 1, 2)), dma((nt - 1, 2)),
            dma((ni - 1,)), dma((ni - 1,)),
            dma((ni - 1,)), dma((ni - 1,)),
            dma((ni - 1,)), dma((ni - 1,)),
            dma((nt - 1,)), dma((nt - 1,)),
            dma((nh - 1,)), dma((nh - 1,)),
            dma((2,)), dma((1,)), dma((1,)),
        ],
        compiler_params=pltpu.CompilerParams(
            collective_id=0, has_side_effects=True, vmem_limit_bytes=60 * 1024 * 1024
        ),
    )(image_feats, key_weight, value_weight, queries, grad_out, mask)
    return (attn.reshape(text, width), grad_feats)


def solution(mesh):
    sizes = (mesh.shape["img"], mesh.shape["head"], mesh.shape["txt"])
    placed = (
        P(("img", "txt"), "head"),
        P("head", None),
        P("head", None),
        P("txt", "head"),
        P("txt", "head"),
        P("img"),
        P(),
    )
    return jax.shard_map(
        functools.partial(shards, sizes),
        mesh=mesh,
        in_specs=placed,
        out_specs=(P("txt", "head"), P(("img", "txt"), "head")),
        check_vma=False,
    )
```
